32 devices in a mesh: groups: 2 (over x), blk: 8 (over z, y), rows: 2 (over core).
Axes of the slice: x: 2, y: 2, z: 4, core: 2. Of those that a mesh axis runs over, the one named last changes fastest.
Arguments:
- features: bfloat16 [8, 16, 256, 512], P('groups', 'rows', 'blk'), parts along dimension 0, may hold values from -60 to 60
- gain_in: float32 [512], replicated, may hold values from 0.25 to 1.75
- shift_in: float32 [512], replicated, may hold values from -3 to 3
- conv_first: bfloat16 [3, 3, 512, 256], replicated, may hold values from -0.09375 to 0.09375
- bias_first: float32 [256], replicated, may hold values from -3 to 3
- short_weight: bfloat16 [512, 256], replicated, may hold values from -0.25 to 0.25
- short_bias: float32 [256], replicated, may hold values from -3 to 3
- gains_rest: float32 [5, 256], replicated, may hold values from 0.25 to 1.75
- shifts_rest: float32 [5, 256], replicated, may hold values from -3 to 3
- convs_rest: bfloat16 [5, 3, 3, 256, 256], replicated, may hold values from -0.125 to 0.125
- biases_rest: float32 [5, 256], replicated, may hold values from -3 to 3
Outputs:
- decoded: bfloat16 [8, 16, 256, 256], P('groups', 'rows', 'blk'), parts along dimension 0
The draws below stay inside these ranges and needn't reach their ends.
There are 2 independent parts, one for each index of `groups`. The reference program is written for one: setup_inputs(seed, part) draws one part's arguments, and reference() takes and returns one part's arrays. A program takes and returns all parts, laid end to end along the dimension named above; an argument that names none is the same for every part. Nothing has to cross between parts.
All inputs are finite; a program needn't handle non-finite values.
Results may differ from the reference program's by a relative error of at most 0.0065.
Values may be sent and summed in bfloat16 or wider, within the bound.
A program may use at most 128 MiB of HBM per device.

```python
import math
import jax
import jax.numpy as jnp
from jax import lax

CH_IN = 512
CH = 256
GROUPS = 32
RESNETS = 3
IMAGES = 4
ROWS_ALL = 16
COLS_ALL = 256


def draw_features(key, part):
    keys = jax.random.split(jax.random.fold_in(key, 17), 5)
    shape = (IMAGES, ROWS_ALL, COLS_ALL, CH_IN)
    base = jax.random.normal(keys[0], shape, jnp.float32)
    rise = math.log(6.0)
    chan_scale = jnp.exp(jax.random.uniform(keys[1], (CH_IN,), jnp.float32, 0.0, math.log(10.0)))
    chan_mean = 0.8 * jax.random.normal(keys[2], (CH_IN,), jnp.float32)
    position = jnp.arange(COLS_ALL, dtype=jnp.float32) / COLS_ALL
    column_scale = jnp.exp(rise * position + jax.random.uniform(keys[3], (COLS_ALL,), jnp.float32, 0.0, math.log(2.0)))
    row_scale = jnp.exp(jax.random.uniform(keys[4], (ROWS_ALL,), jnp.float32, 0.0, math.log(2.0)))
    values = (base + chan_mean) * chan_scale * column_scale[None, None, :, None] * row_scale[None, :, None, None] * 0.15
    return jnp.clip(values, -60.0, 60.0).astype(jnp.bfloat16)


def gaussian(key, shape, width, most, kind=jnp.bfloat16):
    values = width * jax.random.normal(key, shape, jnp.float32)
    return jnp.clip(values, min=-most, max=most).astype(kind)


def setup_inputs(seed: int = 0, part: int = 0) -> dict:
    key_of = jax.random.split(jax.random.key(seed), 12)
    part_keys = jax.random.split(jax.random.fold_in(key_of[11], part), 12)
    features = draw_features(jax.random.fold_in(jax.random.fold_in(key_of[11], part), 71), part)
    gain_in = jnp.clip(1.0 + 0.15 * jax.random.normal(key_of[1], (CH_IN,), jnp.float32), 0.25, 1.75)
    shift_in = gaussian(key_of[2], (CH_IN,), 0.4, 3.0, jnp.float32)
    conv_first = gaussian(key_of[3], (3, 3, CH_IN, CH), (9 * CH_IN) ** -0.5, 0.09375)
    bias_first = gaussian(key_of[4], (CH,), 0.4, 3.0, jnp.float32)
    short_weight = gaussian(key_of[5], (CH_IN, CH), CH_IN ** -0.5, 0.25)
    short_bias = gaussian(key_of[6], (CH,), 0.4, 3.0, jnp.float32)
    gains_rest = jnp.clip(1.0 + 0.15 * jax.random.normal(key_of[7], (2 * RESNETS - 1, CH), jnp.float32), 0.25, 1.75)
    shifts_rest = gaussian(key_of[8], (2 * RESNETS - 1, CH), 0.4, 3.0, jnp.float32)
    convs_rest = gaussian(key_of[9], (2 * RESNETS - 1, 3, 3, CH, CH), (9 * CH) ** -0.5, 0.125)
    biases_rest = gaussian(key_of[10], (2 * RESNETS - 1, CH), 0.4, 3.0, jnp.float32)
    return dict(features=features, gain_in=gain_in, shift_in=shift_in, conv_first=conv_first, bias_first=bias_first, short_weight=short_weight, short_bias=short_bias, gains_rest=gains_rest, shifts_rest=shifts_rest, convs_rest=convs_rest, biases_rest=biases_rest)


EPS = 1e-06

def norm_act(values, gain, shift):
    count = values.shape[3] // GROUPS
    grouped = values.reshape(values.shape[0], values.shape[1], values.shape[2], GROUPS, count)
    center = lax.optimization_barrier(jnp.mean(grouped, axis=(1, 2, 4), keepdims=True))
    spread = lax.optimization_barrier(jnp.mean(jnp.square(grouped - center), axis=(1, 2, 4), keepdims=True))
    scaled = ((grouped - center) * lax.rsqrt(spread + EPS)).reshape(values.shape) * gain + shift
    return (scaled * jax.nn.sigmoid(scaled)).astype(jnp.bfloat16)

def convolve(field, weight, bias):
    wrapped = jnp.concatenate([field[:, :, -1:], field, field[:, :, :1]], axis=2)
    padded = jnp.pad(wrapped, ((0, 0), (1, 1), (0, 0), (0, 0)))
    result = lax.conv_general_dilated(padded.astype(jnp.float32), weight.astype(jnp.float32), (1, 1), 'VALID', dimension_numbers=('NHWC', 'HWIO', 'NHWC'), precision=lax.Precision.HIGHEST)
    return result + bias

def reference(features, gain_in, shift_in, conv_first, bias_first, short_weight, short_bias, gains_rest, shifts_rest, convs_rest, biases_rest):
    stream = features
    for block in range(RESNETS):
        if block == 0:
            first = (gain_in, shift_in, conv_first, bias_first)
        else:
            first = (gains_rest[2 * block - 1], shifts_rest[2 * block - 1], convs_rest[2 * block - 1], biases_rest[2 * block - 1])
        second = (gains_rest[2 * block], shifts_rest[2 * block], convs_rest[2 * block], biases_rest[2 * block])
        active = norm_act(stream.astype(jnp.float32), first[0], first[1])
        inner = convolve(active, first[2], first[3]).astype(jnp.bfloat16)
        active_two = norm_act(inner.astype(jnp.float32), second[0], second[1])
        branch = convolve(active_two, second[2], second[3])
        if block == 0:
            flat = stream.reshape(-1, stream.shape[3])
            skip = jnp.dot(flat, short_weight, preferred_element_type=jnp.float32) + short_bias
            skip = skip.reshape(stream.shape[0], stream.shape[1], stream.shape[2], short_weight.shape[1])
        else:
            skip = stream.astype(jnp.float32)
        stream = (skip + branch).astype(jnp.bfloat16)
    return stream
```

```python
import functools

import jax
import jax.numpy as jnp
from jax import lax
from jax.experimental import pallas as pl
from jax.experimental.pallas import tpu as pltpu
from jax.sharding import PartitionSpec as P

GROUPS = 32
RESNETS = 3
STAGES = 2 * RESNETS
LANES = 128
EPS = 1e-06
MESH = pl.DeviceIdType.MESH


def lane_group_sum(rows, size):
    lane = lax.broadcasted_iota(jnp.int32, rows.shape, 1)
    step = 1
    while step < size:
        ahead = pltpu.roll(rows, LANES - step, 1)
        behind = pltpu.roll(rows, step, 1)
        rows = rows + jnp.where((lane & step) == 0, ahead, behind)
        step *= 2
    return rows


def slot_mask(size):
    lane = lax.broadcasted_iota(jnp.int32, (8, LANES), 1)
    sub = lax.broadcasted_iota(jnp.int32, (8, LANES), 0)
    return (lane & (size - 1)) == sub


def kernel(
    nblk,
    nrow,
    features,
    gain_in,
    shift_in,
    conv_first,
    bias_first,
    short_weight,
    short_bias,
    gains_rest,
    shifts_rest,
    convs_rest,
    biases_rest,
    out,
    feat,
    g0,
    h0,
    w0,
    b0,
    sw,
    sb,
    gr,
    hr,
    wr,
    br,
    inner,
    stream,
    skip,
    act0,
    act1,
    rows0,
    rows1,
    cols0,
    cols1,
    corn0,
    corn1,
    scol0,
    scol1,
    scor0,
    scor1,
    stats,
    load_sem,
    out_sem,
    send_sem,
    recv_sem,
):
    images, height, width, cin = feat.shape
    ch = stream.shape[3]
    ndev = nblk * nrow
    blk = lax.axis_index("blk")
    row = lax.axis_index("rows")
    me = blk * nrow + row
    right = lax.rem(blk + 1, nblk)
    left = lax.rem(blk + nblk - 1, nblk)
    other = 1 - row
    edge = (height - 1) * other
    halo_at = (height + 1) * other
    zero_at = (height + 1) * row

    def device(k):
        target = lax.rem(me + k, ndev)
        return {"blk": target // nrow, "rows": lax.rem(target, nrow)}

    barrier = pltpu.get_barrier_semaphore()

    def greet(k, carry):
        pl.semaphore_signal(barrier, inc=1, device_id=device(k), device_id_type=MESH)
        return carry

    lax.fori_loop(1, ndev, greet, 0)

    loads = []

    def load(src, dst):
        copy = pltpu.make_async_copy(src, dst, load_sem.at[len(loads)])
        copy.start()
        loads.append(copy)
        return copy

    load_feat = [load(features.at[i], feat.at[i]) for i in range(images)]
    load_small = [
        load(a, b)
        for a, b in (
            (gain_in, g0),
            (shift_in, h0),
            (bias_first, b0),
            (short_bias, sb),
            (gains_rest, gr),
            (shifts_rest, hr),
            (biases_rest, br),
        )
    ]
    load_short = load(short_weight, sw)
    load_conv = [load(conv_first, w0)]
    for s in range(1, STAGES):
        load_conv.append(load(convs_rest.at[s - 1], wr.at[s - 1]))

    def transfers(s, i, source):
        if s == 0:
            rbuf, cbuf, nbuf = rows0.at[i], cols0.at[i], corn0.at[i]
            sc, sn = scol0.at[i], scor0.at[i]
        else:
            rbuf, cbuf, nbuf = rows1.at[s - 1, i], cols1.at[s - 1, i], corn1.at[s - 1, i]
            sc, sn = scol1.at[s - 1, i], scor1.at[s - 1, i]

        def remote(src, dst, kind, to):
            return pltpu.make_async_remote_copy(
                src_ref=src,
                dst_ref=dst,
                send_sem=send_sem.at[kind, s, i],
                recv_sem=recv_sem.at[kind, s, i],
                device_id=to,
                device_id_type=MESH,
            )

        halo = [
            remote(source.at[i, edge], rbuf, 0, {"rows": other}),
            remote(sc.at[1], cbuf.at[0], 1, {"blk": right}),
            remote(sc.at[0], cbuf.at[1], 1, {"blk": left}),
            remote(sn.at[1], nbuf.at[0], 2, {"blk": right, "rows": other}),
            remote(sn.at[0], nbuf.at[1], 2, {"blk": left, "rows": other}),
        ]
        mine = stats.at[s, i, me]

        def stat(k):
            return remote(mine, mine, 3, device(k))

        part = stats.at[s, i, pl.ds(0, ndev - 1)]
        waits = [
            remote(source.at[i, edge], rbuf, 0, {"rows": other}),
            remote(sc, cbuf, 1, {"blk": right}),
            remote(sn, nbuf, 2, {"blk": right, "rows": other}),
            remote(part, part, 3, {"rows": other}),
        ]
        return halo, stat, waits

    def publish(s, i, source, values):
        channels = values.shape[1]
        blocks = channels // LANES
        size = channels // GROUPS
        sc = scol0.at[i] if s == 0 else scol1.at[s - 1, i]
        sn = scor0.at[i] if s == 0 else scor1.at[s - 1, i]
        total = jnp.sum(values, axis=0, keepdims=True)
        square = jnp.sum(values * values, axis=0, keepdims=True)
        for r in range(height):
            sc[0, r : r + 1, :] = values[r * width : r * width + 1]
            sc[1, r : r + 1, :] = values[(r + 1) * width - 1 : (r + 1) * width]
        last = (height - 1) * width
        top = jnp.full((1, channels), row, jnp.int32) == 1
        sn[0] = jnp.where(top, values[0:1], values[last : last + 1])
        sn[1] = jnp.where(top, values[width - 1 : width], values[last + width - 1 : last + width])
        pieces = [total[:, b * LANES : (b + 1) * LANES] for b in range(blocks)]
        pieces += [square[:, b * LANES : (b + 1) * LANES] for b in range(blocks)]
        if len(pieces) < 8:
            pieces.append(jnp.zeros((8 - len(pieces), LANES), jnp.float32))
        table = lane_group_sum(jnp.concatenate(pieces, axis=0), size)
        packed = jnp.sum(jnp.where(slot_mask(size), table, 0.0), axis=0, keepdims=True)
        stats[s, i, me] = packed
        return transfers(s, i, source)

    def start(moves):
        halo, stat, _ = moves

        def one(k, carry):
            stat(k).start()
            return carry

        lax.fori_loop(1, ndev, one, 0)
        for copy in halo:
            copy.start()

    def coefficients(s, i, channels, gain, shift):
        blocks = channels // LANES
        size = channels // GROUPS
        count = height * width * ndev * size
        total = jnp.sum(stats[s, i], axis=0)
        table = jnp.where(slot_mask(size), jnp.broadcast_to(total, (8, LANES)), 0.0)
        table = lane_group_sum(table, size) * (1.0 / count)
        center = jnp.concatenate([table[b : b + 1] for b in range(blocks)], axis=1)
        square = jnp.concatenate([table[blocks + b : blocks + b + 1] for b in range(blocks)], axis=1)
        scale = 0.5 * lax.rsqrt(square - center * center + EPS) * gain
        return scale, 0.5 * shift - center * scale

    def activate(s, i, source, gain, shift):
        channels = source.shape[3]
        act = act0 if s == 0 else act1
        rbuf = rows0.at[i] if s == 0 else rows1.at[s - 1, i]
        cbuf = cols0.at[i] if s == 0 else cols1.at[s - 1, i]
        nbuf = corn0.at[i] if s == 0 else corn1.at[s - 1, i]
        scale, offset = coefficients(s, i, channels, gain, shift)

        def silu(x):
            half = x.astype(jnp.float32) * scale + offset
            return half + half * jnp.tanh(half)

        line = lax.broadcasted_iota(jnp.int32, (width, channels), 0)

        def put(at, x, low, high):
            y = silu(x)
            act[at, :, 0:channels] = jnp.where(line == 0, low, pltpu.roll(y, 1, 0)).astype(jnp.bfloat16)
            act[at, :, channels : 2 * channels] = y.astype(jnp.bfloat16)
            act[at, :, 2 * channels : 3 * channels] = jnp.where(
                line == width - 1, high, pltpu.roll(y, width - 1, 0)
            ).astype(jnp.bfloat16)

        low = silu(cbuf[0])
        high = silu(cbuf[1])
        for r in range(height):
            put(r + 1, source[i, r], low[r : r + 1], high[r : r + 1])
        put(halo_at, rbuf[...], silu(nbuf[0]), silu(nbuf[1]))

    def convolve(s):
        act = act0 if s == 0 else act1
        weight = w0[...] if s == 0 else wr[s - 1]
        taps = act.shape[2]
        field = jnp.concatenate(
            [act[d : d + height].reshape(height * width, taps) for d in range(3)], axis=1
        )
        return jnp.dot(field, weight, preferred_element_type=jnp.float32)

    act0[zero_at] = jnp.zeros(act0.shape[1:], act0.dtype)
    act1[zero_at] = jnp.zeros(act1.shape[1:], act1.dtype)

    for i in range(images):
        load_feat[i].wait()
        moves = publish(0, i, feat, feat[i].reshape(height * width, cin).astype(jnp.float32))
        if i == 0:
            pl.semaphore_wait(barrier, ndev - 1)
        start(moves)

    for copy in load_small:
        copy.wait()
    load_short.wait()

    def shortcut(i, carry):
        flat = feat[i].reshape(height * width, cin)
        skip[i] = jnp.dot(flat, sw[...], preferred_element_type=jnp.float32) + sb[...]
        return carry

    lax.fori_loop(0, images, shortcut, 0)

    for s in range(STAGES):
        load_conv[s].wait()
        source = feat if s == 0 else (inner if s % 2 == 1 else stream)
        target = inner if s % 2 == 0 else stream

        def step(i, carry, s=s, source=source, target=target):
            for copy in transfers(s, i, source)[2]:
                copy.wait()
            if s == 0:
                gain, shift, bias = g0[...], h0[...], b0[...]
            else:
                gain, shift, bias = gr[s - 1 : s], hr[s - 1 : s], br[s - 1 : s]
            activate(s, i, source, gain, shift)
            value = convolve(s) + bias
            if s == 1:
                value = value + skip[i]
            elif s % 2 == 1:
                value = value + stream[i].reshape(height * width, ch).astype(jnp.float32)
            rounded = value.astype(jnp.bfloat16)
            target[i] = rounded.reshape(height, width, ch)
            if s + 1 < STAGES:
                start(publish(s + 1, i, target, rounded.astype(jnp.float32)))
            else:
                pltpu.make_async_copy(stream.at[i], out.at[i], out_sem.at[i]).start()
            return carry

        lax.fori_loop(0, images, step, 0)

    for i in range(images):
        pltpu.make_async_copy(stream.at[i], out.at[i], out_sem.at[i]).wait()


def body(nblk, nrow, features, gain_in, shift_in, conv_first, bias_first, short_weight,
         short_bias, gains_rest, shifts_rest, convs_rest, biases_rest):
    images, height, width, cin = features.shape
    ch = conv_first.shape[3]
    rest = STAGES - 1
    ndev = nblk * nrow
    f32, bf16 = jnp.float32, jnp.bfloat16
    args = (
        features,
        gain_in.reshape(1, cin),
        shift_in.reshape(1, cin),
        conv_first.reshape(9 * cin, ch),
        bias_first.reshape(1, ch),
        short_weight,
        short_bias.reshape(1, ch),
        gains_rest,
        shifts_rest,
        convs_rest.reshape(rest, 9 * ch, ch),
        biases_rest,
    )
    anywhere = pl.BlockSpec(memory_space=pl.ANY)
    scratch = [pltpu.VMEM(a.shape, a.dtype) for a in args]
    scratch += [
        pltpu.VMEM((images, height, width, ch), bf16),
        pltpu.VMEM((images, height, width, ch), bf16),
        pltpu.VMEM((images, height * width, ch), f32),
        pltpu.VMEM((height + 2, width, 3 * cin), bf16),
        pltpu.VMEM((height + 2, width, 3 * ch), bf16),
        pltpu.VMEM((images, width, cin), bf16),
        pltpu.VMEM((rest, images, width, ch), bf16),
        pltpu.VMEM((images, 2, height, cin), f32),
        pltpu.VMEM((rest, images, 2, height, ch), f32),
        pltpu.VMEM((images, 2, 1, cin), f32),
        pltpu.VMEM((rest, images, 2, 1, ch), f32),
        pltpu.VMEM((images, 2, height, cin), f32),
        pltpu.VMEM((rest, images, 2, height, ch), f32),
        pltpu.VMEM((images, 2, 1, cin), f32),
        pltpu.VMEM((rest, images, 2, 1, ch), f32),
        pltpu.VMEM((STAGES, images, ndev, 1, LANES), f32),
        pltpu.SemaphoreType.DMA((images + 8 + STAGES,)),
        pltpu.SemaphoreType.DMA((images,)),
        pltpu.SemaphoreType.DMA((4, STAGES, images)),
        pltpu.SemaphoreType.DMA((4, STAGES, images)),
    ]
    return pl.pallas_call(
        functools.partial(kernel, nblk, nrow),
        out_shape=jax.ShapeDtypeStruct((images, height, width, ch), bf16),
        in_specs=[anywhere] * len(args),
        out_specs=anywhere,
        scratch_shapes=scratch,
        compiler_params=pltpu.CompilerParams(
            collective_id=0, has_side_effects=True, vmem_limit_bytes=48 * 1024 * 1024
        ),
    )(*args)


def solution(mesh):
    nblk, nrow = mesh.shape["blk"], mesh.shape["rows"]
    assert nrow == 2
    placed = (P("groups", "rows", "blk", None),) + (P(),) * 10
    return jax.shard_map(
        functools.partial(body, nblk, nrow),
        mesh=mesh,
        in_specs=placed,
        out_specs=P("groups", "rows", "blk", None),
        check_vma=False,
    )
```

```python
import functools

import jax
import jax.numpy as jnp
from jax import lax
from jax.experimental import pallas as pl
from jax.experimental.pallas import tpu as pltpu
from jax.sharding import PartitionSpec as P

GROUPS = 32
RESNETS = 3
STAGES = 2 * RESNETS
LANES = 128
EPS = 1e-06
MESH = pl.DeviceIdType.MESH


def lane_group_sum(rows, size):
    lane = lax.broadcasted_iota(jnp.int32, rows.shape, 1)
    step = 1
    while step < size:
        ahead = pltpu.roll(rows, LANES - step, 1)
        behind = pltpu.roll(rows, step, 1)
        rows = rows + jnp.where((lane & step) == 0, ahead, behind)
        step *= 2
    return rows


def slot_mask(size):
    lane = lax.broadcasted_iota(jnp.int32, (8, LANES), 1)
    sub = lax.broadcasted_iota(jnp.int32, (8, LANES), 0)
    return (lane & (size - 1)) == sub


def kernel(
    nblk,
    nrow,
    features,
    gain_in,
    shift_in,
    conv_first,
    bias_first,
    short_weight,
    short_bias,
    gains_rest,
    shifts_rest,
    convs_rest,
    biases_rest,
    out,
    feat,
    g0,
    h0,
    w0,
    b0,
    sw,
    sb,
    gr,
    hr,
    wr,
    br,
    inner,
    stream,
    skip,
    act0,
    act1,
    rows0,
    rows1,
    cols0,
    cols1,
    corn0,
    corn1,
    scol0,
    scol1,
    scor0,
    scor1,
    stats,
    load_sem,
    out_sem,
    send_sem,
    recv_sem,
):
    images, height, width, cin = feat.shape
    ch = stream.shape[3]
    ndev = nblk * nrow
    blk = lax.axis_index("blk")
    row = lax.axis_index("rows")
    me = blk * nrow + row
    right = lax.rem(blk + 1, nblk)
    left = lax.rem(blk + nblk - 1, nblk)
    other = 1 - row
    edge = (height - 1) * other

    def device(k):
        target = lax.rem(me + k, ndev)
        return {"blk": target // nrow, "rows": lax.rem(target, nrow)}

    barrier = pltpu.get_barrier_semaphore()

    def greet(k, carry):
        pl.semaphore_signal(barrier, inc=1, device_id=device(k), device_id_type=MESH)
        return carry

    lax.fori_loop(1, ndev, greet, 0)

    loads = []

    def load(src, dst):
        copy = pltpu.make_async_copy(src, dst, load_sem.at[len(loads)])
        copy.start()
        loads.append(copy)
        return copy

    load_feat = [load(features.at[i], feat.at[i]) for i in range(images)]
    load_small = [
        load(a, b)
        for a, b in (
            (gain_in, g0),
            (shift_in, h0),
            (bias_first, b0),
            (short_bias, sb),
            (gains_rest, gr),
            (shifts_rest, hr),
            (biases_rest, br),
        )
    ]
    load_short = load(short_weight, sw)
    load_conv = [load(conv_first, w0)]
    for s in range(1, STAGES):
        load_conv.append(load(convs_rest.at[s - 1], wr.at[s - 1]))

    def transfers(s, i, source):
        if s == 0:
            rbuf, cbuf, nbuf = rows0.at[i], cols0.at[i], corn0.at[i]
            sc, sn = scol0.at[i], scor0.at[i]
        else:
            rbuf, cbuf, nbuf = rows1.at[s - 1, i], cols1.at[s - 1, i], corn1.at[s - 1, i]
            sc, sn = scol1.at[s - 1, i], scor1.at[s - 1, i]

        def remote(src, dst, kind, to):
            return pltpu.make_async_remote_copy(
                src_ref=src,
                dst_ref=dst,
                send_sem=send_sem.at[kind, s, i],
                recv_sem=recv_sem.at[kind, s, i],
                device_id=to,
                device_id_type=MESH,
            )

        def halo():
            return [
                remote(sc.at[1], cbuf.at[0], 1, {"blk": right}),
                remote(sc.at[0], cbuf.at[1], 1, {"blk": left}),
                remote(sn.at[1], nbuf.at[0], 2, {"blk": right, "rows": other}),
                remote(sn.at[0], nbuf.at[1], 2, {"blk": left, "rows": other}),
                remote(source.at[i, edge], rbuf, 0, {"rows": other}),
            ]

        mine = stats.at[s, i, me]

        def stat(k):
            return remote(mine, mine, 3, device(k))

        part = stats.at[s, i, pl.ds(0, ndev - 1)]

        def waits():
            return [
                remote(source.at[i, edge], rbuf, 0, {"rows": other}),
                remote(sc, cbuf, 1, {"blk": right}),
                remote(sn, nbuf, 2, {"blk": right, "rows": other}),
                remote(part, part, 3, {"rows": other}),
            ]

        return halo, stat, waits

    def publish(s, i, source, values, entry=None):
        channels = values.shape[1]
        blocks = channels // LANES
        size = channels // GROUPS
        sc = scol0.at[i] if s == 0 else scol1.at[s - 1, i]
        sn = scor0.at[i] if s == 0 else scor1.at[s - 1, i]
        total = jnp.sum(values, axis=0, keepdims=True)
        square = jnp.sum(values * values, axis=0, keepdims=True)
        pieces = [total[:, b * LANES : (b + 1) * LANES] for b in range(blocks)]
        pieces += [square[:, b * LANES : (b + 1) * LANES] for b in range(blocks)]
        if len(pieces) < 8:
            pieces.append(jnp.zeros((8 - len(pieces), LANES), jnp.float32))
        table = lane_group_sum(jnp.concatenate(pieces, axis=0), size)
        packed = jnp.sum(jnp.where(slot_mask(size), table, 0.0), axis=0, keepdims=True)
        stats[s, i, me] = packed
        halo, stat, _ = transfers(s, i, source)
        if entry is not None:
            entry()

        for k in sorted(range(1, ndev), key=lambda k: abs(k - ndev // 2)):
            stat(k).start()
        for r in range(height):
            sc[0, r : r + 1, :] = values[r * width : r * width + 1]
            sc[1, r : r + 1, :] = values[(r + 1) * width - 1 : (r + 1) * width]
        last = (height - 1) * width
        top = jnp.full((1, channels), row, jnp.int32) == 1
        sn[0] = jnp.where(top, values[0:1], values[last : last + 1])
        sn[1] = jnp.where(top, values[width - 1 : width], values[last + width - 1 : last + width])
        for copy in halo():
            copy.start()

    def coefficients(s, i, channels, gain, shift):
        blocks = channels // LANES
        size = channels // GROUPS
        count = height * width * ndev * size
        total = jnp.sum(stats[s, i], axis=0)
        table = jnp.where(slot_mask(size), jnp.broadcast_to(total, (8, LANES)), 0.0)
        table = lane_group_sum(table, size) * (1.0 / count)
        center = jnp.concatenate([table[b : b + 1] for b in range(blocks)], axis=1)
        square = jnp.concatenate([table[blocks + b : blocks + b + 1] for b in range(blocks)], axis=1)
        scale = 0.5 * lax.rsqrt(square - center * center + EPS) * gain
        return scale, 0.5 * shift - center * scale

    def activate(s, i, source, gain, shift):
        channels = source.shape[3]
        act = act0 if s == 0 else act1
        rbuf = rows0.at[i] if s == 0 else rows1.at[s - 1, i]
        cbuf = cols0.at[i] if s == 0 else cols1.at[s - 1, i]
        nbuf = corn0.at[i] if s == 0 else corn1.at[s - 1, i]
        scale, offset = coefficients(s, i, channels, gain, shift)

        def silu(x):
            half = x.astype(jnp.float32) * scale + offset
            return half + half * jnp.tanh(half)

        line = lax.broadcasted_iota(jnp.int32, (width, channels), 0)

        def three(x, low, high):
            y = silu(x)
            return (
                jnp.where(line == 0, low, pltpu.roll(y, 1, 0)),
                y,
                jnp.where(line == width - 1, high, pltpu.roll(y, width - 1, 0)),
            )

        low = silu(cbuf[0])
        high = silu(cbuf[1])
        outer = three(rbuf[...], silu(nbuf[0]), silu(nbuf[1]))
        above = jnp.where(row == 1, 1.0, 0.0)
        for d, piece in enumerate(outer):
            at = pl.ds(d * channels, channels)
            act[0, :, at] = (piece * above).astype(jnp.bfloat16)
            act[height + 1, :, at] = (piece * (1.0 - above)).astype(jnp.bfloat16)
        for r in range(height):
            for d, piece in enumerate(three(source[i, r], low[r : r + 1], high[r : r + 1])):
                act[r + 1, :, pl.ds(d * channels, channels)] = piece.astype(jnp.bfloat16)

    def convolve(s):
        act = act0 if s == 0 else act1
        weight = w0[...] if s == 0 else wr[s - 1]
        taps = act.shape[2]
        field = jnp.concatenate(
            [act[d : d + height].reshape(height * width, taps) for d in range(3)], axis=1
        )
        return jnp.dot(field, weight, preferred_element_type=jnp.float32)

    for i in range(images):
        load_feat[i].wait()
        values = feat[i].reshape(height * width, cin).astype(jnp.float32)
        publish(0, i, feat, values, functools.partial(pl.semaphore_wait, barrier, ndev - 1) if i == 0 else None)

    for copy in load_small:
        copy.wait()
    load_short.wait()

    def shortcut(i, carry):
        flat = feat[i].reshape(height * width, cin)
        skip[i] = jnp.dot(flat, sw[...], preferred_element_type=jnp.float32) + sb[...]
        return carry

    lax.fori_loop(0, images, shortcut, 0)

    for s in range(STAGES):
        load_conv[s].wait()
        source = feat if s == 0 else (inner if s % 2 == 1 else stream)
        target = inner if s % 2 == 0 else stream

        def step(i, carry, s=s, source=source, target=target):
            for copy in transfers(s, i, source)[2]():
                copy.wait()
            if s == 0:
                gain, shift, bias = g0[...], h0[...], b0[...]
            else:
                gain, shift, bias = gr[s - 1 : s], hr[s - 1 : s], br[s - 1 : s]
            activate(s, i, source, gain, shift)
            value = convolve(s) + bias
            if s == 1:
                value = value + skip[i]
            elif s % 2 == 1:
                value = value + stream[i].reshape(height * width, ch).astype(jnp.float32)
            rounded = value.astype(jnp.bfloat16)
            target[i] = rounded.reshape(height, width, ch)
            if s + 1 < STAGES:
                publish(s + 1, i, target, rounded.astype(jnp.float32))
            else:
                pltpu.make_async_copy(stream.at[i], out.at[i], out_sem.at[i]).start()
            return carry

        lax.fori_loop(0, images, step, 0)

    for i in range(images):
        pltpu.make_async_copy(stream.at[i], out.at[i], out_sem.at[i]).wait()


def body(nblk, nrow, features, gain_in, shift_in, conv_first, bias_first, short_weight,
         short_bias, gains_rest, shifts_rest, convs_rest, biases_rest):
    images, height, width, cin = features.shape
    ch = conv_first.shape[3]
    rest = STAGES - 1
    ndev = nblk * nrow
    f32, bf16 = jnp.float32, jnp.bfloat16
    args = (
        features,
        gain_in.reshape(1, cin),
        shift_in.reshape(1, cin),
        conv_first.reshape(9 * cin, ch),
        bias_first.reshape(1, ch),
        short_weight,
        short_bias.reshape(1, ch),
        gains_rest,
        shifts_rest,
        convs_rest.reshape(rest, 9 * ch, ch),
        biases_rest,
    )
    anywhere = pl.BlockSpec(memory_space=pl.ANY)
    scratch = [pltpu.VMEM(a.shape, a.dtype) for a in args]
    scratch += [
        pltpu.VMEM((images, height, width, ch), bf16),
        pltpu.VMEM((images, height, width, ch), bf16),
        pltpu.VMEM((images, height * width, ch), f32),
        pltpu.VMEM((height + 2, width, 3 * cin), bf16),
        pltpu.VMEM((height + 2, width, 3 * ch), bf16),
        pltpu.VMEM((images, width, cin), bf16),
        pltpu.VMEM((rest, images, width, ch), bf16),
        pltpu.VMEM((images, 2, height, cin), f32),
        pltpu.VMEM((rest, images, 2, height, ch), f32),
        pltpu.VMEM((images, 2, 1, cin), f32),
        pltpu.VMEM((rest, images, 2, 1, ch), f32),
        pltpu.VMEM((images, 2, height, cin), f32),
        pltpu.VMEM((rest, images, 2, height, ch), f32),
        pltpu.VMEM((images, 2, 1, cin), f32),
        pltpu.VMEM((rest, images, 2, 1, ch), f32),
        pltpu.VMEM((STAGES, images, ndev, 1, LANES), f32),
        pltpu.SemaphoreType.DMA((images + 8 + STAGES,)),
        pltpu.SemaphoreType.DMA((images,)),
        pltpu.SemaphoreType.DMA((4, STAGES, images)),
        pltpu.SemaphoreType.DMA((4, STAGES, images)),
    ]
    return pl.pallas_call(
        functools.partial(kernel, nblk, nrow),
        out_shape=jax.ShapeDtypeStruct((images, height, width, ch), bf16),
        in_specs=[anywhere] * len(args),
        out_specs=anywhere,
        scratch_shapes=scratch,
        compiler_params=pltpu.CompilerParams(
            collective_id=0, has_side_effects=True, vmem_limit_bytes=67043328
        ),
    )(*args)


def solution(mesh):
    nblk, nrow = mesh.shape["blk"], mesh.shape["rows"]
    assert nrow == 2
    placed = (P("groups", "rows", "blk", None),) + (P(),) * 10
    return jax.shard_map(
        functools.partial(body, nblk, nrow),
        mesh=mesh,
        in_specs=placed,
        out_specs=P("groups", "rows", "blk", None),
        check_vma=False,
    )
```
